32 devices in a mesh: freq: 4 (over y, core), space: 8 (over z, x).
Axes of the slice: x: 2, y: 2, z: 4, core: 2. Of those that a mesh axis runs over, the one named last changes fastest.
Arguments:
- reflection: float32 [2, 32, 1024, 1024], P(None, 'freq', 'space'), may hold values from -6 to 6
- phase: float32 [32, 1024], P('freq'), may hold values from -3.140625 to 3.140625
- group_index: int32 [32], P('freq'), may hold values from 0 to 3
- widths: int32 [8, 2], P('space'), may hold values from 1 to 128
Outputs:
- corrected: float32 [2, 4, 1024, 1024], P(None, 'freq', None, 'space')
The draws below stay inside these ranges and needn't reach their ends.
Inputs may be any that keep to these rules, and one draw needn't show every extreme that they name: `group_index`: each frequency belongs to one depth group. `widths`: margins of a patch are at most one column block wide.
All inputs are finite; a program needn't handle non-finite values.
Results may differ from the reference program's by a relative error of at most 0.0003.
Values sent between devices are 32-bit elements; how exact they have to be, the bound alone decides.
No kernel may reach another device: no remote copies, remote signals or barrier semaphores. Data moves between devices by JAX's collectives and lax.ppermute only.
A program may use at most 64 MiB of HBM per device.

```python
import jax
import jax.numpy as jnp
from jax import lax

N = 1024
ITERS = 3
NF = 32
GROUPS = 4
CB = 128
PATCHES = 8
N_SPACE = 8


def set_ends(result, rng, low, top_value):
    longest = result.shape.index(max(result.shape))
    spots = []
    for shift in (0, 1):
        where = [jax.random.randint(jax.random.fold_in(rng, axis), (), 0, length) for axis, length in enumerate(result.shape)]
        where[longest] = (where[longest] + shift) % result.shape[longest]
        spots.append(tuple(where))
    return result.at[spots[0]].set(low).at[spots[1]].set(top_value)


def block_levels(own_key, extent, cuts, low, largest):
    def one(axis_at, shards_of):
        draws = jax.random.uniform(jax.random.fold_in(jax.random.fold_in(own_key, 6), axis_at), (shards_of,), jnp.float32, low / len(cuts), largest / len(cuts))
        return jnp.repeat(jnp.exp(draws), extent[axis_at] // shards_of).reshape((-1,) + (1,) * (len(extent) - axis_at - 1))

    level = one(*cuts[0])
    for cut in cuts[1:]:
        level = level * one(*cut)
    return level


def bell_draw(stream_key, shape, spread, reach, pieces=(), kind=jnp.bfloat16):
    drawn = jax.random.normal(stream_key, shape, jnp.float32) * spread
    if len(pieces) > 0:
        drawn = block_levels(stream_key, shape, pieces, -0.22, 0.18) * drawn
    return jnp.clip(drawn, min=-reach, max=reach).astype(kind)


def setup_inputs(seed: int = 0) -> dict:
    key_list = jax.random.split(jax.random.key(seed), 5)
    return {
        "reflection": bell_draw(key_list[0], (2, NF, N, N), 1.0, 6.0, ((1, 4), (2, 8)), jnp.float32),
        "phase": jnp.clip(jax.random.uniform(key_list[1], (NF, N), jnp.float32, -3.140625, 3.140625), -3.140625, 3.140625),
        "group_index": set_ends(jax.random.randint(key_list[2], (NF,), 0, GROUPS), jax.random.fold_in(key_list[2], 1), 0, GROUPS - 1).astype(jnp.int32),
        "widths": set_ends(jax.random.randint(key_list[3], (PATCHES, 2), 1, CB + 1), jax.random.fold_in(key_list[3], 1), 1, CB).astype(jnp.int32),
    }


def normalize(real_part, imag_part):
    power = real_part * real_part + imag_part * imag_part
    scale = 1.0 / jnp.sqrt(power + lax.optimization_barrier(jnp.mean(power, axis=0, keepdims=True)) + 1e-06)
    return (real_part * scale, imag_part * scale)

def reference(reflection, phase, group_index, widths):
    width = reflection.shape[2]
    block = width // N_SPACE
    group_ids = jnp.arange(GROUPS, dtype=jnp.int32)

    def add_one(total, index):
        plane_r = lax.dynamic_index_in_dim(reflection[0], index, 0, keepdims=False)
        plane_i = lax.dynamic_index_in_dim(reflection[1], index, 0, keepdims=False)
        angle = lax.dynamic_index_in_dim(phase, index, 0, keepdims=False)
        cosine = jnp.cos(angle)[None, :]
        sine = jnp.sin(angle)[None, :]
        turned = jnp.stack([plane_r * cosine - plane_i * sine, plane_r * sine + plane_i * cosine])
        label = lax.dynamic_index_in_dim(group_index, index, 0, keepdims=False)
        onehot = (group_ids == label).astype(jnp.float32)
        return (total + onehot[:, None, None, None] * turned[None], None)
    start = jnp.zeros((GROUPS, 2, width, width), jnp.float32)
    focused, _ = lax.scan(add_one, start, jnp.arange(NF, dtype=jnp.int32))
    position = jnp.arange(block, dtype=jnp.int32)
    left_keep = (position[None, :] >= block - widths[:, 0:1]).astype(jnp.float32)
    right_keep = (position[None, :] < widths[:, 1:2]).astype(jnp.float32)
    root = jnp.sqrt(jnp.float32(width))
    results = []
    for group in range(GROUPS):
        field = focused[group, 0] + 1j * focused[group, 1]
        spectrum = jnp.fft.fft(jnp.fft.fft(field, axis=1) / root, axis=0) / root
        whole_r = jnp.real(spectrum).astype(jnp.float32).reshape(width, N_SPACE, block)
        whole_i = jnp.imag(spectrum).astype(jnp.float32).reshape(width, N_SPACE, block)
        patch_r = jnp.concatenate([jnp.roll(whole_r, 1, axis=1) * left_keep, whole_r, jnp.roll(whole_r, -1, axis=1) * right_keep], axis=2)
        patch_i = jnp.concatenate([jnp.roll(whole_i, 1, axis=1) * left_keep, whole_i, jnp.roll(whole_i, -1, axis=1) * right_keep], axis=2)
        vector_r, vector_i = normalize(lax.optimization_barrier(jnp.sum(patch_r, axis=2)), lax.optimization_barrier(jnp.sum(patch_i, axis=2)))
        for step in range(ITERS):
            back_r = jnp.einsum('rjc,rj->jc', patch_r, vector_r, precision=lax.Precision.HIGHEST) + jnp.einsum('rjc,rj->jc', patch_i, vector_i, precision=lax.Precision.HIGHEST)
            back_i = jnp.einsum('rjc,rj->jc', patch_r, vector_i, precision=lax.Precision.HIGHEST) - jnp.einsum('rjc,rj->jc', patch_i, vector_r, precision=lax.Precision.HIGHEST)
            next_r = jnp.einsum('rjc,jc->rj', patch_r, back_r, precision=lax.Precision.HIGHEST) - jnp.einsum('rjc,jc->rj', patch_i, back_i, precision=lax.Precision.HIGHEST)
            next_i = jnp.einsum('rjc,jc->rj', patch_r, back_i, precision=lax.Precision.HIGHEST) + jnp.einsum('rjc,jc->rj', patch_i, back_r, precision=lax.Precision.HIGHEST)
            vector_r, vector_i = normalize(next_r, next_i)
        fixed_r = vector_r[:, :, None] * whole_r + vector_i[:, :, None] * whole_i
        fixed_i = vector_r[:, :, None] * whole_i - vector_i[:, :, None] * whole_r
        results.append(jnp.stack([fixed_r.reshape(width, width), fixed_i.reshape(width, width)]))
    return jnp.stack(results, axis=1)
```

```python
import math

import jax
import jax.numpy as jnp
import numpy as np
from jax import lax
from jax.experimental import pallas as pl
from jax.experimental.pallas import tpu as pltpu
from jax.sharding import PartitionSpec as P

ITERS = 3
F32 = jnp.float32
BF16 = jnp.bfloat16


def padded(array, sides, width):
    for axis, dim in sides:
        devices, length = (lax.axis_size(axis), array.shape[dim])
        up = [(i, (i + 1) % devices) for i in range(devices)]
        down = [(j, i) for i, j in up]
        last = lax.slice_in_dim(array, length - width, length, axis=dim)
        leading = lax.slice_in_dim(array, 0, width, axis=dim)
        before = lax.ppermute(last, axis, up)
        after = lax.ppermute(leading, axis, down)
        array = jnp.concatenate([before, array, after], axis=dim)
    return array


def factor_tables(length):
    first = 1
    for divisor in range(1, math.isqrt(length) + 1):
        if length % divisor == 0:
            first = divisor
    second = length // first
    scale = 1.0 / math.sqrt(length)
    outer_a = jnp.arange(first, dtype=jnp.int32)
    outer_b = jnp.arange(second, dtype=jnp.int32)
    angle_a = (outer_a[:, None] * outer_a[None, :] % first).astype(jnp.float32) * (
        -2.0 * math.pi / first
    )
    angle_t = (outer_a[:, None] * outer_b[None, :] % length).astype(jnp.float32) * (
        -2.0 * math.pi / length
    )
    angle_b = (outer_b[:, None] * outer_b[None, :] % second).astype(jnp.float32) * (
        -2.0 * math.pi / second
    )
    return (
        jnp.cos(angle_a) * scale,
        jnp.sin(angle_a) * scale,
        jnp.cos(angle_t),
        jnp.sin(angle_t),
        jnp.cos(angle_b),
        jnp.sin(angle_b),
    )


def hmul(left, right):
    return jnp.matmul(
        left, right, precision=lax.Precision.HIGHEST, preferred_element_type=jnp.float32
    )


def heinsum(form, left, right):
    return jnp.einsum(
        form, left, right, precision=lax.Precision.HIGHEST, preferred_element_type=jnp.float32
    )


def complex_mix(form, real_part, imag_part, table_r, table_i):
    out_r = heinsum(form, real_part, table_r) - heinsum(form, imag_part, table_i)
    out_i = heinsum(form, real_part, table_i) + heinsum(form, imag_part, table_r)
    return (out_r, out_i)


def columns_transform(real_part, imag_part, tables):
    first_r, first_i, twist_r, twist_i, second_r, second_i = tables
    shape = real_part.shape
    first = first_r.shape[0]
    second = second_r.shape[0]
    split_r = real_part.reshape(shape[:-1] + (first, second))
    split_i = imag_part.reshape(shape[:-1] + (first, second))
    mid_r, mid_i = complex_mix("...ab,ak->...kb", split_r, split_i, first_r, first_i)
    turn_r = mid_r * twist_r - mid_i * twist_i
    turn_i = mid_r * twist_i + mid_i * twist_r
    out_r, out_i = complex_mix("...kb,bm->...mk", turn_r, turn_i, second_r, second_i)
    return (out_r.reshape(shape), out_i.reshape(shape))


def rows_transform(real_part, imag_part, tables):
    first_r, first_i, twist_r, twist_i, second_r, second_i = tables
    shape = real_part.shape
    first = first_r.shape[0]
    second = second_r.shape[0]
    split_r = real_part.reshape((first, second) + shape[1:])
    split_i = imag_part.reshape((first, second) + shape[1:])
    mid_r, mid_i = complex_mix("abc,ak->kbc", split_r, split_i, first_r, first_i)
    turn_r = mid_r * twist_r[:, :, None] - mid_i * twist_i[:, :, None]
    turn_i = mid_r * twist_i[:, :, None] + mid_i * twist_r[:, :, None]
    out_r, out_i = complex_mix("kbc,bm->mkc", turn_r, turn_i, second_r, second_i)
    return (out_r.reshape(shape), out_i.reshape(shape))


def normalize(real_part, imag_part):
    power = real_part * real_part + imag_part * imag_part
    scale = 1.0 / jnp.sqrt(power + jnp.mean(power) + 1e-06)
    return (real_part * scale, imag_part * scale)


def plain_local(reflection, phase, group_index, widths):
    width = reflection.shape[3]
    count = lax.axis_size("freq")
    spaces = lax.axis_size("space")
    block = width // spaces
    rows_here = reflection.shape[2]
    cosine = jnp.cos(phase)[:, None, :]
    sine = jnp.sin(phase)[:, None, :]
    turned_r = reflection[0] * cosine - reflection[1] * sine
    turned_i = reflection[0] * sine + reflection[1] * cosine
    onehot = (group_index[:, None] == jnp.arange(count, dtype=jnp.int32)[None, :]).astype(
        jnp.float32
    )
    partial_r = jnp.einsum("fg,frn->grn", onehot, turned_r, precision=lax.Precision.HIGHEST)
    partial_i = jnp.einsum("fg,frn->grn", onehot, turned_i, precision=lax.Precision.HIGHEST)
    tables = factor_tables(width)
    summed = lax.psum_scatter(
        jnp.stack([partial_r, partial_i], axis=1), "freq", scatter_dimension=0, tiled=True
    )
    focus_r = summed[0, 0]
    focus_i = summed[0, 1]
    focus_r, focus_i = columns_transform(focus_r, focus_i, tables)
    blocks = jnp.stack([focus_r, focus_i]).reshape(2, rows_here, spaces, block)
    received = lax.all_to_all(blocks, "space", split_axis=2, concat_axis=1, tiled=True)
    piece_r = received[0, :, 0, :]
    piece_i = received[1, :, 0, :]
    out_r, out_i = rows_transform(piece_r, piece_i, tables)
    owned = jnp.stack([out_r, out_i])
    patch = padded(owned, (("space", 2),), block)
    position = jnp.arange(block, dtype=jnp.int32)
    left_keep = (position >= block - widths[0, 0]).astype(jnp.float32)
    right_keep = (position < widths[0, 1]).astype(jnp.float32)
    keep = jnp.concatenate([left_keep, jnp.ones((block,), jnp.float32), right_keep])
    patch_r = patch[0] * keep[None, :]
    patch_i = patch[1] * keep[None, :]
    vector_r, vector_i = normalize(jnp.sum(patch_r, axis=1), jnp.sum(patch_i, axis=1))
    for step in range(ITERS):
        back_r = hmul(vector_r, patch_r) + hmul(vector_i, patch_i)
        back_i = hmul(vector_i, patch_r) - hmul(vector_r, patch_i)
        next_r = hmul(patch_r, back_r) - hmul(patch_i, back_i)
        next_i = hmul(patch_r, back_i) + hmul(patch_i, back_r)
        vector_r, vector_i = normalize(next_r, next_i)
    own_r = patch[0][:, block : 2 * block]
    own_i = patch[1][:, block : 2 * block]
    fixed_r = vector_r[:, None] * own_r + vector_i[:, None] * own_i
    fixed_i = vector_r[:, None] * own_i - vector_i[:, None] * own_r
    return jnp.stack([fixed_r, fixed_i])[:, None]


def exact_trig(table):
    top, n = table
    angle = -2.0 * np.pi * (top % n) / n
    return np.cos(angle), np.sin(angle)


def halves(values):
    kind = jnp.dtype(BF16)
    high = values.astype(np.float32).astype(kind)
    low = (values - high.astype(np.float64)).astype(np.float32).astype(kind)
    return jnp.asarray(high), jnp.asarray(low)


def dft_tables(width):
    quarter = width // 4
    index = np.arange(quarter)
    real, imag = exact_trig((np.outer(index, index), quarter))
    stack = np.concatenate([real, imag], axis=0) / math.sqrt(width)
    high, low = halves(stack)
    twist = [exact_trig((index * k, width)) for k in range(4)]
    turn = np.concatenate([np.stack([t[0] for t in twist]), np.stack([t[1] for t in twist])], axis=0)
    return high, low, jnp.asarray(turn, F32)


def split(value):
    high = value.astype(BF16)
    return high, (value - high.astype(F32)).astype(BF16)


def transform_into(parts_r, parts_i, high_ref, low_ref, turn_ref, put):
    a_r, b_r, c_r, d_r = parts_r
    a_i, b_i, c_i, d_i = parts_i
    m = a_r.shape[0]
    quarter = a_r.shape[1]
    s0_r, s0_i = a_r + c_r, a_i + c_i
    s1_r, s1_i = a_r - c_r, a_i - c_i
    s2_r, s2_i = b_r + d_r, b_i + d_i
    s3_r, s3_i = b_r - d_r, b_i - d_i
    mixed = (
        (s0_r + s2_r, s0_i + s2_i),
        (s1_r + s3_i, s1_i - s3_r),
        (s0_r - s2_r, s0_i - s2_i),
        (s1_r - s3_i, s1_i + s3_r),
    )
    high = high_ref[...]
    low = low_ref[...]
    dims = (((1,), (1,)), ((), ()))
    for k in range(4):
        v_r, v_i = mixed[k]
        if k > 0:
            t_r = turn_ref[k : k + 1, :]
            t_i = turn_ref[4 + k : 5 + k, :]
            v_r, v_i = v_r * t_r - v_i * t_i, v_r * t_i + v_i * t_r
        both = jnp.concatenate([v_r, v_i], axis=0)
        x_high, x_low = split(both)
        out = lax.dot_general(high, x_high, dims, preferred_element_type=F32)
        out += lax.dot_general(high, x_low, dims, preferred_element_type=F32)
        out += lax.dot_general(low, x_high, dims, preferred_element_type=F32)
        real = out[:quarter, :m] - out[quarter:, m:]
        imag = out[:quarter, m:] + out[quarter:, :m]
        put(k, real, imag)


def turn_kernel(slot_ref, phase_ref, refl_ref, out0, out1, out2, out3, cos_ref, sin_ref):
    @pl.when(pl.program_id(0) == 0)
    def _():
        cos_ref[...] = jnp.cos(phase_ref[...])
        sin_ref[...] = jnp.sin(phase_ref[...])

    outs = (out0, out1, out2, out3)
    for ref in outs:
        ref[...] = jnp.zeros(ref.shape, F32)
    count = refl_ref.shape[1]
    rows = refl_ref.shape[2]
    for f in range(count):
        slot = slot_ref[f]

        def add_to(ref, f=f):
            cosine = cos_ref[f : f + 1, :]
            sine = sin_ref[f : f + 1, :]
            for t in range(0, rows, 8):
                real = refl_ref[0, f, t : t + 8, :]
                imag = refl_ref[1, f, t : t + 8, :]
                ref[0, t : t + 8, :] += real * cosine - imag * sine
                ref[1, t : t + 8, :] += real * sine + imag * cosine

        for value in range(4):

            @pl.when(slot == value)
            def _(value=value):
                add_to(outs[value])


def turn_sum(reflection, phase, slots, rows_at):
    _, count, rows, width = reflection.shape
    shape = jax.ShapeDtypeStruct((2, rows, width), F32)
    spec = pl.BlockSpec((2, rows_at, width), lambda i: (0, i, 0))
    return pl.pallas_call(
        turn_kernel,
        grid=(rows // rows_at,),
        in_specs=[
            pl.BlockSpec(memory_space=pltpu.SMEM),
            pl.BlockSpec((count, width), lambda i: (0, 0)),
            pl.BlockSpec((2, count, rows_at, width), lambda i: (0, 0, i, 0)),
        ],
        out_specs=[spec] * 4,
        out_shape=[shape] * 4,
        scratch_shapes=[pltpu.VMEM((count, width), F32), pltpu.VMEM((count, width), F32)],
        name="turn_sum",
    )(slots, phase, reflection)


def columns_kernel(place_ref, high_ref, low_ref, turn_ref, own_ref, core_ref, far_ref, *refs):
    outs = refs[:-1]
    z_ref = refs[-1]
    width = own_ref.shape[2]
    quarter = width // 4
    spaces = len(outs)
    block = width // spaces

    def plane(p):
        return [
            own_ref[p, :, a * quarter : (a + 1) * quarter]
            + core_ref[p, :, a * quarter : (a + 1) * quarter]
            + far_ref[p, :, a * quarter : (a + 1) * quarter]
            for a in range(4)
        ]

    def put(k, real, imag):
        z_ref[0, pl.ds(k, quarter, stride=4), :] = real
        z_ref[1, pl.ds(k, quarter, stride=4), :] = imag

    transform_into(plane(0), plane(1), high_ref, low_ref, turn_ref, put)
    place = place_ref[0]
    for k in range(spaces):
        start = pl.multiple_of((place ^ k) * block, block)
        outs[k][...] = z_ref[:, pl.ds(start, block), :]


def columns_step(place, tables, own, core, far, spaces):
    _, rows, width = own.shape
    block = width // spaces
    return pl.pallas_call(
        columns_kernel,
        in_specs=[pl.BlockSpec(memory_space=pltpu.SMEM)] + [pl.BlockSpec(memory_space=pltpu.VMEM)] * 6,
        out_specs=[pl.BlockSpec(memory_space=pltpu.VMEM)] * spaces,
        out_shape=[jax.ShapeDtypeStruct((2, block, rows), F32)] * spaces,
        scratch_shapes=[pltpu.VMEM((2, width, rows), F32)],
        name="columns_step",
    )(place, *tables, own, core, far)


def rows_kernel(place_ref, high_ref, low_ref, turn_ref, *refs):
    out_ref, gather_ref = refs[-2:]
    pieces = refs[:-2]
    spaces = len(pieces)
    width = out_ref.shape[1]
    quarter = width // 4
    place = place_ref[0]
    for k in range(spaces):
        gather_ref[place ^ k] = pieces[k][...]
    each = spaces // 4

    def plane(p):
        return [
            jnp.concatenate([gather_ref[a * each + e, p] for e in range(each)], axis=1) for a in range(4)
        ]

    def put(k, real, imag):
        out_ref[0, pl.ds(k, quarter, stride=4), :] = real
        out_ref[1, pl.ds(k, quarter, stride=4), :] = imag

    transform_into(plane(0), plane(1), high_ref, low_ref, turn_ref, put)


def rows_step(place, tables, pieces):
    spaces = len(pieces)
    _, block, rows = pieces[0].shape
    width = rows * spaces
    return pl.pallas_call(
        rows_kernel,
        in_specs=[pl.BlockSpec(memory_space=pltpu.SMEM)] + [pl.BlockSpec(memory_space=pltpu.VMEM)] * (3 + spaces),
        out_specs=pl.BlockSpec(memory_space=pltpu.VMEM),
        out_shape=jax.ShapeDtypeStruct((2, width, block), F32),
        scratch_shapes=[pltpu.VMEM((spaces, 2, block, rows), F32)],
        name="rows_step",
    )(place, *tables, *pieces)


def focus_kernel(widths_ref, before_ref, own_ref, after_ref, out_ref, left_ref, right_ref, back_ref):
    rows, block = own_ref.shape[1:]
    step = 128
    tiles = rows // step
    position = lax.broadcasted_iota(jnp.int32, (1, block), 1)
    left = (position >= block - widths_ref[0, 0]).astype(F32)
    right = (position < widths_ref[0, 1]).astype(F32)

    def masks(t, carry):
        at = pl.ds(pl.multiple_of(t * step, step), step)
        for p in range(2):
            left_ref[p, at, :] = before_ref[p, at, :] * left
            right_ref[p, at, :] = after_ref[p, at, :] * right
        return carry

    lax.fori_loop(0, tiles, masks, 0)
    blocks = (left_ref, own_ref, right_ref)

    def normal(real, imag, total):
        power = real * real + imag * imag
        scale = lax.rsqrt(power + total / rows + 1e-06)
        return real * scale, imag * scale

    def tile(ref, t):
        return ref[0, t * step : (t + 1) * step, :], ref[1, t * step : (t + 1) * step, :]

    def reduce_rows(parts):
        reals, imags = [], []
        total = jnp.zeros((1, 1), F32)
        for real, imag in parts:
            real = jnp.sum(real, axis=1, keepdims=True)
            imag = jnp.sum(imag, axis=1, keepdims=True)
            total = total + jnp.sum(real * real + imag * imag, axis=0, keepdims=True)
            reals.append(real)
            imags.append(imag)
        return [normal(r, i, total) for r, i in zip(reals, imags)]

    def first():
        for t in range(tiles):
            real = left_ref[0, t * step : (t + 1) * step, :]
            imag = left_ref[1, t * step : (t + 1) * step, :]
            for ref in blocks[1:]:
                r, i = tile(ref, t)
                real, imag = real + r, imag + i
            yield real, imag

    vector = reduce_rows(first())
    for _ in range(ITERS):
        back = []
        for ref in blocks:
            back_r = jnp.zeros((8, block), F32)
            back_i = jnp.zeros((8, block), F32)
            for t in range(tiles):
                r, i = tile(ref, t)
                v_r, v_i = vector[t]
                back_r += jnp.sum((r * v_r + i * v_i).reshape(step // 8, 8, block), axis=0)
                back_i += jnp.sum((r * v_i - i * v_r).reshape(step // 8, 8, block), axis=0)
            back.append((jnp.sum(back_r, axis=0, keepdims=True), jnp.sum(back_i, axis=0, keepdims=True)))

        def forward():
            for t in range(tiles):
                real = imag = None
                for ref, (b_r, b_i) in zip(blocks, back):
                    r, i = tile(ref, t)
                    x, y = r * b_r - i * b_i, r * b_i + i * b_r
                    real, imag = (x, y) if real is None else (real + x, imag + y)
                yield real, imag

        vector = reduce_rows(forward())
    for t in range(tiles):
        r, i = tile(own_ref, t)
        v_r, v_i = vector[t]
        out_ref[0, 0, t * step : (t + 1) * step, :] = v_r * r + v_i * i
        out_ref[1, 0, t * step : (t + 1) * step, :] = v_r * i - v_i * r


def focus_step(widths, before, own, after):
    _, rows, block = own.shape
    vmem = pl.BlockSpec(memory_space=pltpu.VMEM)
    return pl.pallas_call(
        focus_kernel,
        in_specs=[pl.BlockSpec(memory_space=pltpu.SMEM), vmem, vmem, vmem],
        out_specs=vmem,
        out_shape=jax.ShapeDtypeStruct((2, 1, rows, block), F32),
        scratch_shapes=[pltpu.VMEM((2, rows, block), F32), pltpu.VMEM((2, rows, block), F32), pltpu.VMEM((8, block), F32)],
        name="focus_step",
    )(widths, before, own, after)


def local(reflection, phase, group_index, widths):
    rows_here, width = reflection.shape[2:]
    count = lax.axis_size("freq")
    spaces = lax.axis_size("space")
    tables = dft_tables(width)
    me = lax.axis_index("freq")
    place = lax.axis_index("space").astype(jnp.int32)[None]
    slots = group_index ^ me
    near = [(i, i ^ 1) for i in range(count)]
    far = [(i, i ^ 2) for i in range(count)]
    own, core, distant, corner = turn_sum(reflection, phase, slots, min(32, rows_here))
    corner = lax.ppermute(corner, "freq", near)
    core = lax.ppermute(core, "freq", near)
    distant = lax.ppermute(distant + corner, "freq", far)
    pieces = columns_step(place, tables, own, core, distant, spaces)
    pieces = [pieces[0]] + [
        lax.ppermute(pieces[k], "space", [(i, i ^ k) for i in range(spaces)]) for k in range(1, spaces)
    ]
    own = rows_step(place, tables, pieces)
    up = [(i, (i + 1) % spaces) for i in range(spaces)]
    down = [(j, i) for i, j in up]
    before = lax.ppermute(own, "space", up)
    after = lax.ppermute(own, "space", down)
    return focus_step(widths, before, own, after)


def solution(mesh):
    in_specs = (P(None, "freq", "space", None), P("freq", None), P("freq"), P("space", None))
    out_specs = P(None, "freq", None, "space")

    def step(reflection, phase, group_index, widths):
        block = reflection.shape[3] // mesh.shape["space"]
        rows = reflection.shape[2] // mesh.shape["space"]
        whole = block % 128 == 0 and rows == 128 and mesh.shape["freq"] == 4 and mesh.shape["space"] == 8
        body = local if whole else plain_local
        return jax.shard_map(
            body, mesh=mesh, in_specs=in_specs, out_specs=out_specs, check_vma=False
        )(reflection, phase, group_index, widths)

    return step
```

```python
import functools
import math

import jax
import jax.numpy as jnp
import numpy as np
from jax import lax
from jax.experimental import pallas as pl
from jax.experimental.pallas import tpu as pltpu
from jax.sharding import PartitionSpec as P


ITERS = 3
F32 = jnp.float32
BF16 = jnp.bfloat16


def padded(array, sides, width):
    for axis, dim in sides:
        devices, length = (lax.axis_size(axis), array.shape[dim])
        up = [(i, (i + 1) % devices) for i in range(devices)]
        down = [(j, i) for i, j in up]
        last = lax.slice_in_dim(array, length - width, length, axis=dim)
        leading = lax.slice_in_dim(array, 0, width, axis=dim)
        before = lax.ppermute(last, axis, up)
        after = lax.ppermute(leading, axis, down)
        array = jnp.concatenate([before, array, after], axis=dim)
    return array


def factor_tables(length):
    first = 1
    for divisor in range(1, math.isqrt(length) + 1):
        if length % divisor == 0:
            first = divisor
    second = length // first
    scale = 1.0 / math.sqrt(length)
    outer_a = jnp.arange(first, dtype=jnp.int32)
    outer_b = jnp.arange(second, dtype=jnp.int32)
    angle_a = (outer_a[:, None] * outer_a[None, :] % first).astype(jnp.float32) * (
        -2.0 * math.pi / first
    )
    angle_t = (outer_a[:, None] * outer_b[None, :] % length).astype(jnp.float32) * (
        -2.0 * math.pi / length
    )
    angle_b = (outer_b[:, None] * outer_b[None, :] % second).astype(jnp.float32) * (
        -2.0 * math.pi / second
    )
    return (
        jnp.cos(angle_a) * scale,
        jnp.sin(angle_a) * scale,
        jnp.cos(angle_t),
        jnp.sin(angle_t),
        jnp.cos(angle_b),
        jnp.sin(angle_b),
    )


def hmul(left, right):
    return jnp.matmul(
        left, right, precision=lax.Precision.HIGHEST, preferred_element_type=jnp.float32
    )


def heinsum(form, left, right):
    return jnp.einsum(
        form, left, right, precision=lax.Precision.HIGHEST, preferred_element_type=jnp.float32
    )


def complex_mix(form, real_part, imag_part, table_r, table_i):
    out_r = heinsum(form, real_part, table_r) - heinsum(form, imag_part, table_i)
    out_i = heinsum(form, real_part, table_i) + heinsum(form, imag_part, table_r)
    return (out_r, out_i)


def columns_transform(real_part, imag_part, tables):
    first_r, first_i, twist_r, twist_i, second_r, second_i = tables
    shape = real_part.shape
    first = first_r.shape[0]
    second = second_r.shape[0]
    split_r = real_part.reshape(shape[:-1] + (first, second))
    split_i = imag_part.reshape(shape[:-1] + (first, second))
    mid_r, mid_i = complex_mix("...ab,ak->...kb", split_r, split_i, first_r, first_i)
    turn_r = mid_r * twist_r - mid_i * twist_i
    turn_i = mid_r * twist_i + mid_i * twist_r
    out_r, out_i = complex_mix("...kb,bm->...mk", turn_r, turn_i, second_r, second_i)
    return (out_r.reshape(shape), out_i.reshape(shape))


def rows_transform(real_part, imag_part, tables):
    first_r, first_i, twist_r, twist_i, second_r, second_i = tables
    shape = real_part.shape
    first = first_r.shape[0]
    second = second_r.shape[0]
    split_r = real_part.reshape((first, second) + shape[1:])
    split_i = imag_part.reshape((first, second) + shape[1:])
    mid_r, mid_i = complex_mix("abc,ak->kbc", split_r, split_i, first_r, first_i)
    turn_r = mid_r * twist_r[:, :, None] - mid_i * twist_i[:, :, None]
    turn_i = mid_r * twist_i[:, :, None] + mid_i * twist_r[:, :, None]
    out_r, out_i = complex_mix("kbc,bm->mkc", turn_r, turn_i, second_r, second_i)
    return (out_r.reshape(shape), out_i.reshape(shape))


def normalize(real_part, imag_part):
    power = real_part * real_part + imag_part * imag_part
    scale = 1.0 / jnp.sqrt(power + jnp.mean(power) + 1e-06)
    return (real_part * scale, imag_part * scale)


def plain_local(reflection, phase, group_index, widths):
    width = reflection.shape[3]
    count = lax.axis_size("freq")
    spaces = lax.axis_size("space")
    block = width // spaces
    rows_here = reflection.shape[2]
    cosine = jnp.cos(phase)[:, None, :]
    sine = jnp.sin(phase)[:, None, :]
    turned_r = reflection[0] * cosine - reflection[1] * sine
    turned_i = reflection[0] * sine + reflection[1] * cosine
    onehot = (group_index[:, None] == jnp.arange(count, dtype=jnp.int32)[None, :]).astype(
        jnp.float32
    )
    partial_r = jnp.einsum("fg,frn->grn", onehot, turned_r, precision=lax.Precision.HIGHEST)
    partial_i = jnp.einsum("fg,frn->grn", onehot, turned_i, precision=lax.Precision.HIGHEST)
    tables = factor_tables(width)
    summed = lax.psum_scatter(
        jnp.stack([partial_r, partial_i], axis=1), "freq", scatter_dimension=0, tiled=True
    )
    focus_r = summed[0, 0]
    focus_i = summed[0, 1]
    focus_r, focus_i = columns_transform(focus_r, focus_i, tables)
    blocks = jnp.stack([focus_r, focus_i]).reshape(2, rows_here, spaces, block)
    received = lax.all_to_all(blocks, "space", split_axis=2, concat_axis=1, tiled=True)
    piece_r = received[0, :, 0, :]
    piece_i = received[1, :, 0, :]
    out_r, out_i = rows_transform(piece_r, piece_i, tables)
    owned = jnp.stack([out_r, out_i])
    patch = padded(owned, (("space", 2),), block)
    position = jnp.arange(block, dtype=jnp.int32)
    left_keep = (position >= block - widths[0, 0]).astype(jnp.float32)
    right_keep = (position < widths[0, 1]).astype(jnp.float32)
    keep = jnp.concatenate([left_keep, jnp.ones((block,), jnp.float32), right_keep])
    patch_r = patch[0] * keep[None, :]
    patch_i = patch[1] * keep[None, :]
    vector_r, vector_i = normalize(jnp.sum(patch_r, axis=1), jnp.sum(patch_i, axis=1))
    for _ in range(ITERS):
        back_r = hmul(vector_r, patch_r) + hmul(vector_i, patch_i)
        back_i = hmul(vector_i, patch_r) - hmul(vector_r, patch_i)
        next_r = hmul(patch_r, back_r) - hmul(patch_i, back_i)
        next_i = hmul(patch_r, back_i) + hmul(patch_i, back_r)
        vector_r, vector_i = normalize(next_r, next_i)
    own_r = patch[0][:, block : 2 * block]
    own_i = patch[1][:, block : 2 * block]
    fixed_r = vector_r[:, None] * own_r + vector_i[:, None] * own_i
    fixed_i = vector_r[:, None] * own_i - vector_i[:, None] * own_r
    return jnp.stack([fixed_r, fixed_i])[:, None]


def unit_angles(top, n):
    angle = -2.0 * np.pi * (top % n) / n
    return np.cos(angle), np.sin(angle)


def halves(values):
    kind = jnp.dtype(BF16)
    high = values.astype(np.float32).astype(kind)
    low = (values - high.astype(np.float64)).astype(np.float32).astype(kind)
    return jnp.asarray(np.concatenate([high, high, low], axis=1))


def quarter_matrix(width):
    quarter = width // 4
    index = np.arange(quarter)
    real, imag = unit_angles(np.outer(index, index), quarter)
    return real / math.sqrt(width), imag / math.sqrt(width)


def column_tables(width):
    quarter = width // 4
    real, imag = quarter_matrix(width)
    twist = [unit_angles(np.arange(quarter) * k, width) for k in range(4)]
    turn = np.stack([t[0] for t in twist] + [t[1] for t in twist])
    return halves(np.concatenate([real, imag], axis=1)), jnp.asarray(turn, F32)


def row_tables(width, chunk, chunks, block):
    part = block // chunks
    lane = np.arange(2 * block)
    imaginary = lane % block >= part
    row = lane // block * block + chunk * part + lane % part
    real, imag = quarter_matrix(width)
    real, imag = real[:, row], imag[:, row]
    upper = np.where(imaginary, -imag, real)
    lower = np.where(imaginary, real, imag)
    twist = [unit_angles(row * k, width) for k in range(4)]
    sign = np.where(imaginary, 1.0, -1.0)
    turn = np.stack([t[0] for t in twist] + [t[1] * sign for t in twist])
    return halves(np.concatenate([upper, lower], axis=0)), jnp.asarray(turn, F32)


def split(value):
    high = value.astype(BF16)
    return high, (value - high.astype(F32)).astype(BF16)


def cost(micros):
    return pl.CostEstimate(flops=int(micros * 8e7), bytes_accessed=0, transcendentals=0)


def product(table, right):
    high, low = split(right)
    sides = jnp.concatenate([high, low, high], axis=1)
    return lax.dot_general(table, sides, (((1,), (1,)), ((), ())), preferred_element_type=F32)


def turn_kernel(me_ref, group_ref, phase_ref, refl_ref, own_ref, far_ref, send_ref, cos_ref, sin_ref, sum_ref):
    @pl.when(pl.program_id(0) == 0)
    def _():
        cos_ref[...] = jnp.cos(phase_ref[...])
        sin_ref[...] = jnp.sin(phase_ref[...])

    sum_ref[...] = jnp.zeros(sum_ref.shape, F32)
    count = refl_ref.shape[1]
    rows = refl_ref.shape[2]
    for f in range(count):
        slot = group_ref[f] ^ me_ref[0]
        cosine = cos_ref[f : f + 1, :]
        sine = sin_ref[f : f + 1, :]
        for t in range(0, rows, 8):
            real = refl_ref[0, f, t : t + 8, :]
            imag = refl_ref[1, f, t : t + 8, :]
            sum_ref[slot, 0, t : t + 8, :] += real * cosine - imag * sine
            sum_ref[slot, 1, t : t + 8, :] += real * sine + imag * cosine
    own_ref[...] = sum_ref[0]
    far_ref[...] = sum_ref[2]
    send_ref[0] = sum_ref[3]
    send_ref[1] = sum_ref[1]


def turn_sum(me, groups, phase, reflection, first, rows, rows_at):
    _, count, _, width = reflection.shape
    shape = jax.ShapeDtypeStruct((2, rows, width), F32)
    spec = pl.BlockSpec((2, rows_at, width), lambda i: (0, i, 0))
    offset = first // rows_at
    return pl.pallas_call(
        turn_kernel,
        grid=(rows // rows_at,),
        in_specs=[
            pl.BlockSpec(memory_space=pltpu.SMEM),
            pl.BlockSpec(memory_space=pltpu.SMEM),
            pl.BlockSpec((count, width), lambda i: (0, 0)),
            pl.BlockSpec((2, count, rows_at, width), lambda i: (0, 0, i + offset, 0)),
        ],
        out_specs=[spec, spec, pl.BlockSpec((2, 2, rows_at, width), lambda i: (0, 0, i, 0))],
        out_shape=[shape, shape, jax.ShapeDtypeStruct((2, 2, rows, width), F32)],
        scratch_shapes=[pltpu.VMEM((count, width), F32)] * 2 + [pltpu.VMEM((4, 2, rows_at, width), F32)],
        name="turn_sum",
        compiler_params=pltpu.CompilerParams(vmem_limit_bytes=57 * 2**20),
        cost_estimate=cost(4),
    )(me, groups, phase, reflection)


def columns_kernel(place_ref, table_ref, turn_ref, own_ref, core_ref, far_ref, *refs):
    outs = refs[:-1]
    z_ref = refs[-1]
    rows, width = own_ref.shape[1:]
    quarter = width // 4
    block = width // (2 * len(outs))

    def plane(p):
        cuts = [slice(a * quarter, (a + 1) * quarter) for a in range(4)]
        return [own_ref[p, :, c] + core_ref[1, p, :, c] + far_ref[p, :, c] for c in cuts]

    a_r, b_r, c_r, d_r = plane(0)
    a_i, b_i, c_i, d_i = plane(1)
    s0_r, s0_i = a_r + c_r, a_i + c_i
    s1_r, s1_i = a_r - c_r, a_i - c_i
    s2_r, s2_i = b_r + d_r, b_i + d_i
    s3_r, s3_i = b_r - d_r, b_i - d_i
    mixed = (
        (s0_r + s2_r, s0_i + s2_i),
        (s1_r + s3_i, s1_i - s3_r),
        (s0_r - s2_r, s0_i - s2_i),
        (s1_r - s3_i, s1_i + s3_r),
    )
    for pair in range(2):
        stacked = []
        for k in (2 * pair, 2 * pair + 1):
            v_r, v_i = mixed[k]
            if k > 0:
                t_r = turn_ref[k : k + 1, :]
                t_i = turn_ref[4 + k : 5 + k, :]
                v_r, v_i = v_r * t_r - v_i * t_i, v_r * t_i + v_i * t_r
            stacked.append(jnp.concatenate([v_r, -v_i], axis=1))
            stacked.append(jnp.concatenate([v_i, v_r], axis=1))
        out = product(table_ref[...], jnp.concatenate(stacked, axis=0))
        for e in range(2):
            z_ref[pl.ds(2 * pair + e, quarter, stride=4), :] = out[:, 2 * rows * e : 2 * rows * (e + 1)]
    place = place_ref[0]
    for k in range(len(outs)):
        for p in range(2):
            start = pl.multiple_of((place ^ (2 * k + p)) * block, block)
            outs[k][p] = z_ref[pl.ds(start, block), :]


def columns_step(place, tables, own, core, far, spaces):
    _, rows, width = own.shape
    block = width // spaces
    return pl.pallas_call(
        columns_kernel,
        in_specs=[pl.BlockSpec(memory_space=pltpu.SMEM)] + [pl.BlockSpec(memory_space=pltpu.VMEM)] * 5,
        out_specs=[pl.BlockSpec(memory_space=pltpu.VMEM)] * (spaces // 2),
        out_shape=[jax.ShapeDtypeStruct((2, block, 2 * rows), F32)] * (spaces // 2),
        scratch_shapes=[pltpu.VMEM((width, 2 * rows), F32)],
        name="columns_step",
        compiler_params=pltpu.CompilerParams(vmem_limit_bytes=12 * 2**20),
        cost_estimate=cost(3),
    )(place, *tables, own, core, far)


def rows_kernel(sides, origin_ref, table_ref, turn_ref, same_ref, cross_ref, *refs):
    out_ref, pieces_ref = refs[-2:]
    spaces, block, _ = pieces_ref.shape
    quarter = out_ref.shape[1] // 4
    origin = origin_ref[0]
    for k in range(spaces // 2):
        pieces_ref[origin ^ (2 * k)] = same_ref[sides[0], k]
        pieces_ref[origin ^ (2 * k + 1)] = cross_ref[sides[1], k]
    half = block // 2
    lane = lax.broadcasted_iota(jnp.int32, (1, block), 1)
    sign = jnp.where(lane < half, 1.0, -1.0)

    def swap(x):
        return pltpu.roll(x, half, 1)

    def piece(s):
        return pieces_ref[s]

    mixed = [[], [], [], []]
    for e in range(2):
        a, b, c, d = [piece(2 * q + e) for q in range(4)]
        s0, s1, s2 = a + c, a - c, b + d
        s3 = swap(b - d) * sign
        for k, v in enumerate((s0 + s2, s1 + s3, s0 - s2, s1 - s3)):
            if k > 0:
                at = slice(e * block, (e + 1) * block)
                v = v * turn_ref[k : k + 1, at] + swap(v) * turn_ref[4 + k : 5 + k, at]
            mixed[k].append(v)
    for pair in range(2):
        stacked = [jnp.concatenate(mixed[k], axis=1) for k in (2 * pair, 2 * pair + 1)]
        out = product(table_ref[...], jnp.concatenate(stacked, axis=0))
        for e in range(2):
            at = pl.ds(2 * pair + e, quarter, stride=4)
            for p in range(2):
                value = out[p * quarter : (p + 1) * quarter, e * block : (e + 1) * block]
                if len(refs) > 2:
                    value = value + refs[0][p, at, :]
                out_ref[p, at, :] = value


def rows_step(origin, tables, sides, same, cross, *sofar):
    _, pairs, block, _ = same.shape
    width = 2 * pairs * block
    return pl.pallas_call(
        functools.partial(rows_kernel, sides),
        in_specs=[pl.BlockSpec(memory_space=pltpu.SMEM)] + [pl.BlockSpec(memory_space=pltpu.VMEM)] * (4 + len(sofar)),
        out_specs=pl.BlockSpec(memory_space=pltpu.VMEM),
        out_shape=jax.ShapeDtypeStruct((2, width, block), F32),
        scratch_shapes=[pltpu.VMEM((2 * pairs, block, block), F32)],
        name="rows_step",
        compiler_params=pltpu.CompilerParams(vmem_limit_bytes=12 * 2**20),
        cost_estimate=cost(1),
    )(origin, *tables, same, cross, *sofar)


def focus_kernel(place_ref, widths_ref, own_ref, near_in, other_in, out_ref, near_ref, other_ref):
    rows, block = own_ref.shape[1:]
    step = 128
    tiles = rows // step
    position = lax.broadcasted_iota(jnp.int32, (1, block), 1)
    near_left = place_ref[0] % 2
    left = (position >= block - widths_ref[0, 0]).astype(jnp.int32)
    right = (position < widths_ref[0, 1]).astype(jnp.int32)
    near = (left * near_left + right * (1 - near_left)).astype(F32)
    other = (right * near_left + left * (1 - near_left)).astype(F32)

    def masks(t, carry):
        at = pl.ds(pl.multiple_of(t * step, step), step)
        for p in range(2):
            near_ref[p, at, :] = near_in[p, at, :] * near
            other_ref[p, at, :] = other_in[p, at, :] * other
        return carry

    lax.fori_loop(0, tiles, masks, 0)
    blocks = (near_ref, own_ref, other_ref)

    def normal(real, imag, total):
        power = real * real + imag * imag
        scale = lax.rsqrt(power + total / rows + 1e-06)
        return real * scale, imag * scale

    def tile(ref, t):
        return ref[0, t * step : (t + 1) * step, :], ref[1, t * step : (t + 1) * step, :]

    def reduce_rows(parts):
        reals, imags = [], []
        total = jnp.zeros((1, 1), F32)
        for real, imag in parts:
            real = jnp.sum(real, axis=1, keepdims=True)
            imag = jnp.sum(imag, axis=1, keepdims=True)
            total = total + jnp.sum(real * real + imag * imag, axis=0, keepdims=True)
            reals.append(real)
            imags.append(imag)
        return [normal(r, i, total) for r, i in zip(reals, imags)]

    def first():
        for t in range(tiles):
            real = near_ref[0, t * step : (t + 1) * step, :]
            imag = near_ref[1, t * step : (t + 1) * step, :]
            for ref in blocks[1:]:
                r, i = tile(ref, t)
                real, imag = real + r, imag + i
            yield real, imag

    vector = reduce_rows(first())
    for _ in range(ITERS):
        back = []
        for ref in blocks:
            back_r = jnp.zeros((8, block), F32)
            back_i = jnp.zeros((8, block), F32)
            for t in range(tiles):
                r, i = tile(ref, t)
                v_r, v_i = vector[t]
                back_r += jnp.sum((r * v_r + i * v_i).reshape(step // 8, 8, block), axis=0)
                back_i += jnp.sum((r * v_i - i * v_r).reshape(step // 8, 8, block), axis=0)
            back.append((jnp.sum(back_r, axis=0, keepdims=True), jnp.sum(back_i, axis=0, keepdims=True)))

        def forward():
            for t in range(tiles):
                real = imag = None
                for ref, (b_r, b_i) in zip(blocks, back):
                    r, i = tile(ref, t)
                    x, y = r * b_r - i * b_i, r * b_i + i * b_r
                    real, imag = (x, y) if real is None else (real + x, imag + y)
                yield real, imag

        vector = reduce_rows(forward())
    for t in range(tiles):
        r, i = tile(own_ref, t)
        v_r, v_i = vector[t]
        out_ref[0, 0, t * step : (t + 1) * step, :] = v_r * r + v_i * i
        out_ref[1, 0, t * step : (t + 1) * step, :] = v_r * i - v_i * r


def focus_step(place, widths, own, near, other):
    _, rows, block = own.shape
    vmem = pl.BlockSpec(memory_space=pltpu.VMEM)
    return pl.pallas_call(
        focus_kernel,
        in_specs=[pl.BlockSpec(memory_space=pltpu.SMEM)] * 2 + [vmem] * 3,
        out_specs=vmem,
        out_shape=jax.ShapeDtypeStruct((2, 1, rows, block), F32),
        scratch_shapes=[pltpu.VMEM((2, rows, block), F32), pltpu.VMEM((2, rows, block), F32)],
        name="focus_step",
        compiler_params=pltpu.CompilerParams(vmem_limit_bytes=16 * 2**20),
        cost_estimate=cost(6),
    )(place, widths, own, near, other)


CHUNKS = 2


def local(reflection, phase, group_index, widths):
    return focus_all(reflection, phase, group_index, widths)


def focus_all(reflection, phase, group_index, widths):
    rows_here, width = reflection.shape[2:]
    count = lax.axis_size("freq")
    spaces = lax.axis_size("space")
    block = width // spaces
    me = lax.axis_index("freq").astype(jnp.int32)[None]
    place = lax.axis_index("space").astype(jnp.int32)[None]
    near = [(i, i ^ 1) for i in range(count)]
    far = [(i, i ^ 2) for i in range(count)]
    along = [(i, (i + 2 if i % 2 == 0 else i - 2) % spaces) for i in range(spaces)]
    beyond_from = jnp.where(place % 2 == 0, place + (spaces - 2), place + 2) % spaces
    columns = column_tables(width)
    chunk = rows_here // CHUNKS
    sums = [turn_sum(me, group_index, phase, reflection, h * chunk, chunk, 32) for h in range(CHUNKS)]
    cores, fars = [], []
    for h in range(CHUNKS):
        cores.append(lax.ppermute(sums[h][2], "freq", near))
        partial = sums[h][1] + cores[h][0]
        fars.append(lax.ppermute(partial, "freq", far))
    own_block = near_block = other_block = ()
    for h in range(CHUNKS):
        rows = row_tables(width, h, CHUNKS, block)
        pieces = list(columns_step(place, columns, sums[h][0], cores[h], fars[h], spaces))
        for k in range(1, spaces // 2):
            pieces[k] = lax.ppermute(pieces[k], "space", [(i, i ^ (2 * k)) for i in range(spaces)])
        same = jnp.stack(pieces, axis=1)
        cross = lax.ppermute(same, "space", [(i, i ^ 1) for i in range(spaces)])
        beyond = lax.ppermute(jnp.stack([same[1], cross[0]]), "space", along)
        own_block = (rows_step(place, rows, (0, 1), same, cross, *own_block),)
        near_block = (rows_step(place, rows, (1, 0), same, cross, *near_block),)
        other_block = (rows_step(beyond_from, rows, (0, 1), beyond, beyond, *other_block),)
    return focus_step(place, widths, own_block[0], near_block[0], other_block[0])


def solution(mesh):
    in_specs = (P(None, "freq", "space", None), P("freq", None), P("freq"), P("space", None))
    out_specs = P(None, "freq", None, "space")

    def step(reflection, phase, group_index, widths):
        block = reflection.shape[3] // mesh.shape["space"]
        rows = reflection.shape[2] // mesh.shape["space"]
        whole = block % 128 == 0 and rows == 128 and mesh.shape["freq"] == 4 and mesh.shape["space"] == 8
        body = local if whole else plain_local
        return jax.shard_map(
            body, mesh=mesh, in_specs=in_specs, out_specs=out_specs, check_vma=False
        )(reflection, phase, group_index, widths)

    return step
```

```python
import math

import jax
import jax.numpy as jnp
import numpy as np
from jax import lax
from jax.experimental import pallas as pl
from jax.experimental.pallas import tpu as pltpu
from jax.sharding import PartitionSpec as P


ITERS = 3
F32 = jnp.float32
BF16 = jnp.bfloat16


def padded(array, sides, width):
    for axis, dim in sides:
        devices, length = (lax.axis_size(axis), array.shape[dim])
        up = [(i, (i + 1) % devices) for i in range(devices)]
        down = [(j, i) for i, j in up]
        last = lax.slice_in_dim(array, length - width, length, axis=dim)
        leading = lax.slice_in_dim(array, 0, width, axis=dim)
        before = lax.ppermute(last, axis, up)
        after = lax.ppermute(leading, axis, down)
        array = jnp.concatenate([before, array, after], axis=dim)
    return array


def factor_tables(length):
    first = 1
    for divisor in range(1, math.isqrt(length) + 1):
        if length % divisor == 0:
            first = divisor
    second = length // first
    scale = 1.0 / math.sqrt(length)
    outer_a = jnp.arange(first, dtype=jnp.int32)
    outer_b = jnp.arange(second, dtype=jnp.int32)
    angle_a = (outer_a[:, None] * outer_a[None, :] % first).astype(jnp.float32) * (
        -2.0 * math.pi / first
    )
    angle_t = (outer_a[:, None] * outer_b[None, :] % length).astype(jnp.float32) * (
        -2.0 * math.pi / length
    )
    angle_b = (outer_b[:, None] * outer_b[None, :] % second).astype(jnp.float32) * (
        -2.0 * math.pi / second
    )
    return (
        jnp.cos(angle_a) * scale,
        jnp.sin(angle_a) * scale,
        jnp.cos(angle_t),
        jnp.sin(angle_t),
        jnp.cos(angle_b),
        jnp.sin(angle_b),
    )


def hmul(left, right):
    return jnp.matmul(
        left, right, precision=lax.Precision.HIGHEST, preferred_element_type=jnp.float32
    )


def heinsum(form, left, right):
    return jnp.einsum(
        form, left, right, precision=lax.Precision.HIGHEST, preferred_element_type=jnp.float32
    )


def complex_mix(form, real_part, imag_part, table_r, table_i):
    out_r = heinsum(form, real_part, table_r) - heinsum(form, imag_part, table_i)
    out_i = heinsum(form, real_part, table_i) + heinsum(form, imag_part, table_r)
    return (out_r, out_i)


def columns_transform(real_part, imag_part, tables):
    first_r, first_i, twist_r, twist_i, second_r, second_i = tables
    shape = real_part.shape
    first = first_r.shape[0]
    second = second_r.shape[0]
    split_r = real_part.reshape(shape[:-1] + (first, second))
    split_i = imag_part.reshape(shape[:-1] + (first, second))
    mid_r, mid_i = complex_mix("...ab,ak->...kb", split_r, split_i, first_r, first_i)
    turn_r = mid_r * twist_r - mid_i * twist_i
    turn_i = mid_r * twist_i + mid_i * twist_r
    out_r, out_i = complex_mix("...kb,bm->...mk", turn_r, turn_i, second_r, second_i)
    return (out_r.reshape(shape), out_i.reshape(shape))


def rows_transform(real_part, imag_part, tables):
    first_r, first_i, twist_r, twist_i, second_r, second_i = tables
    shape = real_part.shape
    first = first_r.shape[0]
    second = second_r.shape[0]
    split_r = real_part.reshape((first, second) + shape[1:])
    split_i = imag_part.reshape((first, second) + shape[1:])
    mid_r, mid_i = complex_mix("abc,ak->kbc", split_r, split_i, first_r, first_i)
    turn_r = mid_r * twist_r[:, :, None] - mid_i * twist_i[:, :, None]
    turn_i = mid_r * twist_i[:, :, None] + mid_i * twist_r[:, :, None]
    out_r, out_i = complex_mix("kbc,bm->mkc", turn_r, turn_i, second_r, second_i)
    return (out_r.reshape(shape), out_i.reshape(shape))


def normalize(real_part, imag_part):
    power = real_part * real_part + imag_part * imag_part
    scale = 1.0 / jnp.sqrt(power + jnp.mean(power) + 1e-06)
    return (real_part * scale, imag_part * scale)


def plain_local(reflection, phase, group_index, widths):
    width = reflection.shape[3]
    count = lax.axis_size("freq")
    spaces = lax.axis_size("space")
    block = width // spaces
    rows_here = reflection.shape[2]
    cosine = jnp.cos(phase)[:, None, :]
    sine = jnp.sin(phase)[:, None, :]
    turned_r = reflection[0] * cosine - reflection[1] * sine
    turned_i = reflection[0] * sine + reflection[1] * cosine
    onehot = (group_index[:, None] == jnp.arange(count, dtype=jnp.int32)[None, :]).astype(
        jnp.float32
    )
    partial_r = jnp.einsum("fg,frn->grn", onehot, turned_r, precision=lax.Precision.HIGHEST)
    partial_i = jnp.einsum("fg,frn->grn", onehot, turned_i, precision=lax.Precision.HIGHEST)
    tables = factor_tables(width)
    summed = lax.psum_scatter(
        jnp.stack([partial_r, partial_i], axis=1), "freq", scatter_dimension=0, tiled=True
    )
    focus_r = summed[0, 0]
    focus_i = summed[0, 1]
    focus_r, focus_i = columns_transform(focus_r, focus_i, tables)
    blocks = jnp.stack([focus_r, focus_i]).reshape(2, rows_here, spaces, block)
    received = lax.all_to_all(blocks, "space", split_axis=2, concat_axis=1, tiled=True)
    piece_r = received[0, :, 0, :]
    piece_i = received[1, :, 0, :]
    out_r, out_i = rows_transform(piece_r, piece_i, tables)
    owned = jnp.stack([out_r, out_i])
    patch = padded(owned, (("space", 2),), block)
    position = jnp.arange(block, dtype=jnp.int32)
    left_keep = (position >= block - widths[0, 0]).astype(jnp.float32)
    right_keep = (position < widths[0, 1]).astype(jnp.float32)
    keep = jnp.concatenate([left_keep, jnp.ones((block,), jnp.float32), right_keep])
    patch_r = patch[0] * keep[None, :]
    patch_i = patch[1] * keep[None, :]
    vector_r, vector_i = normalize(jnp.sum(patch_r, axis=1), jnp.sum(patch_i, axis=1))
    for _ in range(ITERS):
        back_r = hmul(vector_r, patch_r) + hmul(vector_i, patch_i)
        back_i = hmul(vector_i, patch_r) - hmul(vector_r, patch_i)
        next_r = hmul(patch_r, back_r) - hmul(patch_i, back_i)
        next_i = hmul(patch_r, back_i) + hmul(patch_i, back_r)
        vector_r, vector_i = normalize(next_r, next_i)
    own_r = patch[0][:, block : 2 * block]
    own_i = patch[1][:, block : 2 * block]
    fixed_r = vector_r[:, None] * own_r + vector_i[:, None] * own_i
    fixed_i = vector_r[:, None] * own_i - vector_i[:, None] * own_r
    return jnp.stack([fixed_r, fixed_i])[:, None]


def unit_angles(top, n):
    angle = -2.0 * np.pi * (top % n) / n
    return np.cos(angle), np.sin(angle)


def halves(values):
    kind = jnp.dtype(BF16)
    high = values.astype(np.float32).astype(kind)
    low = (values - high.astype(np.float64)).astype(np.float32).astype(kind)
    return jnp.asarray(np.concatenate([high, high, low], axis=1))


def quarter_matrix(width):
    quarter = width // 4
    index = np.arange(quarter)
    real, imag = unit_angles(np.outer(index, index), quarter)
    return real / math.sqrt(width), imag / math.sqrt(width)


def column_tables(width):
    quarter = width // 4
    real, imag = quarter_matrix(width)
    twist = [unit_angles(np.arange(quarter) * k, width) for k in range(4)]
    turn = np.stack([t[0] for t in twist] + [t[1] for t in twist])
    return halves(np.concatenate([real, imag], axis=1)), jnp.asarray(turn, F32)


def row_tables(width, chunk, chunks, block):
    part = block // chunks
    lane = np.arange(2 * block)
    imaginary = lane % block >= part
    row = lane // block * block + chunk * part + lane % part
    real, imag = quarter_matrix(width)
    real, imag = real[:, row], imag[:, row]
    upper = np.where(imaginary, -imag, real)
    lower = np.where(imaginary, real, imag)
    twist = [unit_angles(row * k, width) for k in range(4)]
    sign = np.where(imaginary, 1.0, -1.0)
    turn = np.stack([t[0] for t in twist] + [t[1] * sign for t in twist])
    return halves(np.concatenate([upper, lower], axis=0)), jnp.asarray(turn, F32)


def split(value):
    high = value.astype(BF16)
    return high, (value - high.astype(F32)).astype(BF16)


def cost(micros):
    return pl.CostEstimate(flops=int(micros * 8e7), bytes_accessed=0, transcendentals=0)


def product(table, right):
    high, low = split(right)
    sides = jnp.concatenate([high, low, high], axis=1)
    return lax.dot_general(table, sides, (((1,), (1,)), ((), ())), preferred_element_type=F32)


def turn_kernel(me_ref, group_ref, phase_ref, refl_ref, own_ref, far_ref, send_ref, cos_ref, sin_ref, sum_ref):
    @pl.when(pl.program_id(0) == 0)
    def _():
        cos_ref[...] = jnp.cos(phase_ref[...])
        sin_ref[...] = jnp.sin(phase_ref[...])

    sum_ref[...] = jnp.zeros(sum_ref.shape, F32)
    count = refl_ref.shape[1]
    rows = refl_ref.shape[2]
    for f in range(count):
        slot = group_ref[f] ^ me_ref[0]
        cosine = cos_ref[f : f + 1, :]
        sine = sin_ref[f : f + 1, :]
        for t in range(0, rows, 8):
            real = refl_ref[0, f, t : t + 8, :]
            imag = refl_ref[1, f, t : t + 8, :]
            sum_r = sum_ref[slot, 0, t : t + 8, :]
            sum_i = sum_ref[slot, 1, t : t + 8, :]
            sum_ref[slot, 0, t : t + 8, :] = sum_r + (real * cosine - imag * sine)
            sum_ref[slot, 1, t : t + 8, :] = sum_i + (real * sine + imag * cosine)
    own_ref[...] = sum_ref[0]
    far_ref[...] = sum_ref[2]
    send_ref[0] = sum_ref[3]
    send_ref[1] = sum_ref[1]


def turn_sum(me, groups, phase, reflection, first, rows, rows_at):
    _, count, _, width = reflection.shape
    shape = jax.ShapeDtypeStruct((2, rows, width), F32)
    spec = pl.BlockSpec((2, rows_at, width), lambda i: (0, i, 0))
    offset = first // rows_at
    return pl.pallas_call(
        turn_kernel,
        grid=(rows // rows_at,),
        in_specs=[
            pl.BlockSpec(memory_space=pltpu.SMEM),
            pl.BlockSpec(memory_space=pltpu.SMEM),
            pl.BlockSpec((count, width), lambda i: (0, 0)),
            pl.BlockSpec((2, count, rows_at, width), lambda i: (0, 0, i + offset, 0)),
        ],
        out_specs=[spec, spec, pl.BlockSpec((2, 2, rows_at, width), lambda i: (0, 0, i, 0))],
        out_shape=[shape, shape, jax.ShapeDtypeStruct((2, 2, rows, width), F32)],
        scratch_shapes=[pltpu.VMEM((count, width), F32)] * 2 + [pltpu.VMEM((4, 2, rows_at, width), F32)],
        name="turn_sum",
        compiler_params=pltpu.CompilerParams(vmem_limit_bytes=56 * 2**20),
        cost_estimate=cost(4),
    )(me, groups, phase, reflection)


def columns_kernel(place_ref, table_ref, turn_ref, own_ref, far_ref, *refs):
    outs = refs[:-1]
    z_ref = refs[-1]
    rows, width = own_ref.shape[1:]
    quarter = width // 4
    block = width // (2 * len(outs))

    def plane(p):
        cuts = [slice(a * quarter, (a + 1) * quarter) for a in range(4)]
        return [own_ref[p, :, c] + far_ref[p, :, c] for c in cuts]

    a_r, b_r, c_r, d_r = plane(0)
    a_i, b_i, c_i, d_i = plane(1)
    s0_r, s0_i = a_r + c_r, a_i + c_i
    s1_r, s1_i = a_r - c_r, a_i - c_i
    s2_r, s2_i = b_r + d_r, b_i + d_i
    s3_r, s3_i = b_r - d_r, b_i - d_i
    mixed = (
        (s0_r + s2_r, s0_i + s2_i),
        (s1_r + s3_i, s1_i - s3_r),
        (s0_r - s2_r, s0_i - s2_i),
        (s1_r - s3_i, s1_i + s3_r),
    )
    for pair in range(2):
        stacked = []
        for k in (2 * pair, 2 * pair + 1):
            v_r, v_i = mixed[k]
            if k > 0:
                t_r = turn_ref[k : k + 1, :]
                t_i = turn_ref[4 + k : 5 + k, :]
                v_r, v_i = v_r * t_r - v_i * t_i, v_r * t_i + v_i * t_r
            stacked.append(jnp.concatenate([v_r, -v_i], axis=1))
            stacked.append(jnp.concatenate([v_i, v_r], axis=1))
        out = product(table_ref[...], jnp.concatenate(stacked, axis=0))
        for e in range(2):
            z_ref[pl.ds(2 * pair + e, quarter, stride=4), :] = out[:, 2 * rows * e : 2 * rows * (e + 1)]
    place = place_ref[0]
    for k in range(len(outs)):
        for p in range(2):
            start = pl.multiple_of((place ^ (2 * k + p)) * block, block)
            outs[k][p] = z_ref[pl.ds(start, block), :]


def columns_step(place, tables, own, far, spaces):
    _, rows, width = own.shape
    block = width // spaces
    return pl.pallas_call(
        columns_kernel,
        in_specs=[pl.BlockSpec(memory_space=pltpu.SMEM)] + [pl.BlockSpec(memory_space=pltpu.VMEM)] * 4,
        out_specs=[pl.BlockSpec(memory_space=pltpu.VMEM)] * (spaces // 2),
        out_shape=[jax.ShapeDtypeStruct((2, block, 2 * rows), F32)] * (spaces // 2),
        scratch_shapes=[pltpu.VMEM((width, 2 * rows), F32)],
        name="columns_step",
        compiler_params=pltpu.CompilerParams(vmem_limit_bytes=12 * 2**20),
        cost_estimate=cost(3),
    )(place, *tables, own, far)


def rows_kernel(origin_ref, table_ref, turn_ref, same_ref, cross_ref, *refs):
    out_ref, pieces_ref = refs[-2:]
    spaces, block, _ = pieces_ref.shape
    quarter = out_ref.shape[1] // 4
    origin = origin_ref[0]
    for k in range(spaces // 2):
        pieces_ref[origin ^ (2 * k)] = same_ref[k]
        pieces_ref[origin ^ (2 * k + 1)] = cross_ref[k]
    half = block // 2
    lane = lax.broadcasted_iota(jnp.int32, (1, block), 1)
    sign = jnp.where(lane < half, 1.0, -1.0)

    def swap(x):
        return pltpu.roll(x, half, 1)

    def piece(s):
        return pieces_ref[s]

    mixed = [[], [], [], []]
    for e in range(2):
        a, b, c, d = [piece(2 * q + e) for q in range(4)]
        s0, s1, s2 = a + c, a - c, b + d
        s3 = swap(b - d) * sign
        for k, v in enumerate((s0 + s2, s1 + s3, s0 - s2, s1 - s3)):
            if k > 0:
                at = slice(e * block, (e + 1) * block)
                v = v * turn_ref[k : k + 1, at] + swap(v) * turn_ref[4 + k : 5 + k, at]
            mixed[k].append(v)
    for pair in range(2):
        stacked = [jnp.concatenate(mixed[k], axis=1) for k in (2 * pair, 2 * pair + 1)]
        out = product(table_ref[...], jnp.concatenate(stacked, axis=0))
        for e in range(2):
            at = pl.ds(2 * pair + e, quarter, stride=4)
            for p in range(2):
                value = out[p * quarter : (p + 1) * quarter, e * block : (e + 1) * block]
                if len(refs) > 2:
                    value = value + refs[0][p, at, :]
                out_ref[p, at, :] = value


def rows_step(origin, tables, same, cross, *sofar):
    pairs, block, _ = same.shape
    width = 2 * pairs * block
    return pl.pallas_call(
        rows_kernel,
        in_specs=[pl.BlockSpec(memory_space=pltpu.SMEM)] + [pl.BlockSpec(memory_space=pltpu.VMEM)] * (4 + len(sofar)),
        out_specs=pl.BlockSpec(memory_space=pltpu.VMEM),
        out_shape=jax.ShapeDtypeStruct((2, width, block), F32),
        scratch_shapes=[pltpu.VMEM((2 * pairs, block, block), F32)],
        name="rows_step",
        compiler_params=pltpu.CompilerParams(vmem_limit_bytes=12 * 2**20),
        cost_estimate=cost(1),
    )(origin, *tables, same, cross, *sofar)


def focus_kernel(place_ref, widths_ref, own_ref, near_in, other_in, out_ref, near_ref, other_ref):
    rows, block = own_ref.shape[1:]
    step = 128
    tiles = rows // step
    position = lax.broadcasted_iota(jnp.int32, (1, block), 1)
    near_left = place_ref[0] % 2
    left = (position >= block - widths_ref[0, 0]).astype(jnp.int32)
    right = (position < widths_ref[0, 1]).astype(jnp.int32)
    near = (left * near_left + right * (1 - near_left)).astype(F32)
    other = (right * near_left + left * (1 - near_left)).astype(F32)

    def masks(t, carry):
        at = pl.ds(pl.multiple_of(t * step, step), step)
        for p in range(2):
            near_ref[p, at, :] = near_in[p, at, :] * near
            other_ref[p, at, :] = other_in[p, at, :] * other
        return carry

    lax.fori_loop(0, tiles, masks, 0)
    blocks = (near_ref, own_ref, other_ref)

    def normal(real, imag, total):
        power = real * real + imag * imag
        scale = lax.rsqrt(power + total / rows + 1e-06)
        return real * scale, imag * scale

    def tile(ref, t):
        return ref[0, t * step : (t + 1) * step, :], ref[1, t * step : (t + 1) * step, :]

    def reduce_rows(parts):
        reals, imags = [], []
        total = jnp.zeros((1, 1), F32)
        for real, imag in parts:
            real = jnp.sum(real, axis=1, keepdims=True)
            imag = jnp.sum(imag, axis=1, keepdims=True)
            total = total + jnp.sum(real * real + imag * imag, axis=0, keepdims=True)
            reals.append(real)
            imags.append(imag)
        return [normal(r, i, total) for r, i in zip(reals, imags)]

    def first():
        for t in range(tiles):
            real = near_ref[0, t * step : (t + 1) * step, :]
            imag = near_ref[1, t * step : (t + 1) * step, :]
            for ref in blocks[1:]:
                r, i = tile(ref, t)
                real, imag = real + r, imag + i
            yield real, imag

    vector = reduce_rows(first())
    for _ in range(ITERS):
        back = []
        for ref in blocks:
            back_r = jnp.zeros((8, block), F32)
            back_i = jnp.zeros((8, block), F32)
            for t in range(tiles):
                r, i = tile(ref, t)
                v_r, v_i = vector[t]
                back_r += jnp.sum((r * v_r + i * v_i).reshape(step // 8, 8, block), axis=0)
                back_i += jnp.sum((r * v_i - i * v_r).reshape(step // 8, 8, block), axis=0)
            back.append((jnp.sum(back_r, axis=0, keepdims=True), jnp.sum(back_i, axis=0, keepdims=True)))

        def forward():
            for t in range(tiles):
                real = imag = None
                for ref, (b_r, b_i) in zip(blocks, back):
                    r, i = tile(ref, t)
                    x, y = r * b_r - i * b_i, r * b_i + i * b_r
                    real, imag = (x, y) if real is None else (real + x, imag + y)
                yield real, imag

        vector = reduce_rows(forward())
    for t in range(tiles):
        r, i = tile(own_ref, t)
        v_r, v_i = vector[t]
        out_ref[0, 0, t * step : (t + 1) * step, :] = v_r * r + v_i * i
        out_ref[1, 0, t * step : (t + 1) * step, :] = v_r * i - v_i * r


def focus_step(place, widths, own, near, other):
    _, rows, block = own.shape
    vmem = pl.BlockSpec(memory_space=pltpu.VMEM)
    return pl.pallas_call(
        focus_kernel,
        in_specs=[pl.BlockSpec(memory_space=pltpu.SMEM)] * 2 + [vmem] * 3,
        out_specs=vmem,
        out_shape=jax.ShapeDtypeStruct((2, 1, rows, block), F32),
        scratch_shapes=[pltpu.VMEM((2, rows, block), F32), pltpu.VMEM((2, rows, block), F32)],
        name="focus_step",
        compiler_params=pltpu.CompilerParams(vmem_limit_bytes=16 * 2**20),
        cost_estimate=cost(6),
    )(place, widths, own, near, other)


CHUNKS = 2


def local(reflection, phase, group_index, widths):
    return focus_all(reflection, phase, group_index, widths)


def focus_all(reflection, phase, group_index, widths):
    rows_here, width = reflection.shape[2:]
    count = lax.axis_size("freq")
    spaces = lax.axis_size("space")
    block = width // spaces
    me = lax.axis_index("freq").astype(jnp.int32)[None]
    place = lax.axis_index("space").astype(jnp.int32)[None]
    near = [(i, i ^ 1) for i in range(count)]
    far = [(i, i ^ 2) for i in range(count)]
    along = [(i, (i + 2 if i % 2 == 0 else i - 2) % spaces) for i in range(spaces)]
    beyond_from = jnp.where(place % 2 == 0, place + (spaces - 2), place + 2) % spaces
    columns = column_tables(width)
    chunk = rows_here // CHUNKS
    cores, fars, mine = [], [], []
    sums = []
    for h in range(CHUNKS):
        sums.append(turn_sum(me, group_index, phase, reflection, h * chunk, chunk, 32))
        cores.append(lax.ppermute(sums[h][2], "freq", near))
        partial = sums[h][1] + cores[h][0]
        mine.append(sums[h][0] + cores[h][1])
        fars.append(lax.ppermute(partial, "freq", far))
    own_block = near_block = other_block = ()
    for h in range(CHUNKS):
        rows = row_tables(width, h, CHUNKS, block)
        pieces = list(columns_step(place, columns, mine[h], fars[h], spaces))
        for k in range(1, spaces // 2):
            pieces[k] = lax.ppermute(pieces[k], "space", [(i, i ^ (2 * k)) for i in range(spaces)])
        own_same, near_same = [jnp.stack([piece[p] for piece in pieces]) for p in range(2)]
        across = [(i, i ^ 1) for i in range(spaces)]
        near_cross = lax.ppermute(own_same, "space", across)
        own_cross = lax.ppermute(near_same, "space", across)
        beyond = lax.ppermute(jnp.stack([near_same, near_cross]), "space", along)
        own_block = (rows_step(place, rows, own_same, own_cross, *own_block),)
        near_block = (rows_step(place, rows, near_same, near_cross, *near_block),)
        other_block = (rows_step(beyond_from, rows, beyond[0], beyond[1], *other_block),)
    return focus_step(place, widths, own_block[0], near_block[0], other_block[0])


def solution(mesh):
    in_specs = (P(None, "freq", "space", None), P("freq", None), P("freq"), P("space", None))
    out_specs = P(None, "freq", None, "space")

    def step(reflection, phase, group_index, widths):
        block = reflection.shape[3] // mesh.shape["space"]
        rows = reflection.shape[2] // mesh.shape["space"]
        whole = block % 128 == 0 and rows == 128 and mesh.shape["freq"] == 4 and mesh.shape["space"] == 8
        body = local if whole else plain_local
        return jax.shard_map(
            body, mesh=mesh, in_specs=in_specs, out_specs=out_specs, check_vma=False
        )(reflection, phase, group_index, widths)

    return step
```

```python
import math

import jax
import jax.numpy as jnp
import numpy as np
from jax import lax
from jax.experimental import pallas as pl
from jax.experimental.pallas import tpu as pltpu
from jax.sharding import PartitionSpec as P


ITERS = 3
F32 = jnp.float32
BF16 = jnp.bfloat16


def padded(array, sides, width):
    for axis, dim in sides:
        devices, length = (lax.axis_size(axis), array.shape[dim])
        up = [(i, (i + 1) % devices) for i in range(devices)]
        down = [(j, i) for i, j in up]
        last = lax.slice_in_dim(array, length - width, length, axis=dim)
        leading = lax.slice_in_dim(array, 0, width, axis=dim)
        before = lax.ppermute(last, axis, up)
        after = lax.ppermute(leading, axis, down)
        array = jnp.concatenate([before, array, after], axis=dim)
    return array


def factor_tables(length):
    first = 1
    for divisor in range(1, math.isqrt(length) + 1):
        if length % divisor == 0:
            first = divisor
    second = length // first
    scale = 1.0 / math.sqrt(length)
    outer_a = jnp.arange(first, dtype=jnp.int32)
    outer_b = jnp.arange(second, dtype=jnp.int32)
    angle_a = (outer_a[:, None] * outer_a[None, :] % first).astype(jnp.float32) * (
        -2.0 * math.pi / first
    )
    angle_t = (outer_a[:, None] * outer_b[None, :] % length).astype(jnp.float32) * (
        -2.0 * math.pi / length
    )
    angle_b = (outer_b[:, None] * outer_b[None, :] % second).astype(jnp.float32) * (
        -2.0 * math.pi / second
    )
    return (
        jnp.cos(angle_a) * scale,
        jnp.sin(angle_a) * scale,
        jnp.cos(angle_t),
        jnp.sin(angle_t),
        jnp.cos(angle_b),
        jnp.sin(angle_b),
    )


def hmul(left, right):
    return jnp.matmul(
        left, right, precision=lax.Precision.HIGHEST, preferred_element_type=jnp.float32
    )


def heinsum(form, left, right):
    return jnp.einsum(
        form, left, right, precision=lax.Precision.HIGHEST, preferred_element_type=jnp.float32
    )


def complex_mix(form, real_part, imag_part, table_r, table_i):
    out_r = heinsum(form, real_part, table_r) - heinsum(form, imag_part, table_i)
    out_i = heinsum(form, real_part, table_i) + heinsum(form, imag_part, table_r)
    return (out_r, out_i)


def columns_transform(real_part, imag_part, tables):
    first_r, first_i, twist_r, twist_i, second_r, second_i = tables
    shape = real_part.shape
    first = first_r.shape[0]
    second = second_r.shape[0]
    split_r = real_part.reshape(shape[:-1] + (first, second))
    split_i = imag_part.reshape(shape[:-1] + (first, second))
    mid_r, mid_i = complex_mix("...ab,ak->...kb", split_r, split_i, first_r, first_i)
    turn_r = mid_r * twist_r - mid_i * twist_i
    turn_i = mid_r * twist_i + mid_i * twist_r
    out_r, out_i = complex_mix("...kb,bm->...mk", turn_r, turn_i, second_r, second_i)
    return (out_r.reshape(shape), out_i.reshape(shape))


def rows_transform(real_part, imag_part, tables):
    first_r, first_i, twist_r, twist_i, second_r, second_i = tables
    shape = real_part.shape
    first = first_r.shape[0]
    second = second_r.shape[0]
    split_r = real_part.reshape((first, second) + shape[1:])
    split_i = imag_part.reshape((first, second) + shape[1:])
    mid_r, mid_i = complex_mix("abc,ak->kbc", split_r, split_i, first_r, first_i)
    turn_r = mid_r * twist_r[:, :, None] - mid_i * twist_i[:, :, None]
    turn_i = mid_r * twist_i[:, :, None] + mid_i * twist_r[:, :, None]
    out_r, out_i = complex_mix("kbc,bm->mkc", turn_r, turn_i, second_r, second_i)
    return (out_r.reshape(shape), out_i.reshape(shape))


def normalize(real_part, imag_part):
    power = real_part * real_part + imag_part * imag_part
    scale = 1.0 / jnp.sqrt(power + jnp.mean(power) + 1e-06)
    return (real_part * scale, imag_part * scale)


def plain_local(reflection, phase, group_index, widths):
    width = reflection.shape[3]
    count = lax.axis_size("freq")
    spaces = lax.axis_size("space")
    block = width // spaces
    rows_here = reflection.shape[2]
    cosine = jnp.cos(phase)[:, None, :]
    sine = jnp.sin(phase)[:, None, :]
    turned_r = reflection[0] * cosine - reflection[1] * sine
    turned_i = reflection[0] * sine + reflection[1] * cosine
    onehot = (group_index[:, None] == jnp.arange(count, dtype=jnp.int32)[None, :]).astype(
        jnp.float32
    )
    partial_r = jnp.einsum("fg,frn->grn", onehot, turned_r, precision=lax.Precision.HIGHEST)
    partial_i = jnp.einsum("fg,frn->grn", onehot, turned_i, precision=lax.Precision.HIGHEST)
    tables = factor_tables(width)
    summed = lax.psum_scatter(
        jnp.stack([partial_r, partial_i], axis=1), "freq", scatter_dimension=0, tiled=True
    )
    focus_r = summed[0, 0]
    focus_i = summed[0, 1]
    focus_r, focus_i = columns_transform(focus_r, focus_i, tables)
    blocks = jnp.stack([focus_r, focus_i]).reshape(2, rows_here, spaces, block)
    received = lax.all_to_all(blocks, "space", split_axis=2, concat_axis=1, tiled=True)
    piece_r = received[0, :, 0, :]
    piece_i = received[1, :, 0, :]
    out_r, out_i = rows_transform(piece_r, piece_i, tables)
    owned = jnp.stack([out_r, out_i])
    patch = padded(owned, (("space", 2),), block)
    position = jnp.arange(block, dtype=jnp.int32)
    left_keep = (position >= block - widths[0, 0]).astype(jnp.float32)
    right_keep = (position < widths[0, 1]).astype(jnp.float32)
    keep = jnp.concatenate([left_keep, jnp.ones((block,), jnp.float32), right_keep])
    patch_r = patch[0] * keep[None, :]
    patch_i = patch[1] * keep[None, :]
    vector_r, vector_i = normalize(jnp.sum(patch_r, axis=1), jnp.sum(patch_i, axis=1))
    for _ in range(ITERS):
        back_r = hmul(vector_r, patch_r) + hmul(vector_i, patch_i)
        back_i = hmul(vector_i, patch_r) - hmul(vector_r, patch_i)
        next_r = hmul(patch_r, back_r) - hmul(patch_i, back_i)
        next_i = hmul(patch_r, back_i) + hmul(patch_i, back_r)
        vector_r, vector_i = normalize(next_r, next_i)
    own_r = patch[0][:, block : 2 * block]
    own_i = patch[1][:, block : 2 * block]
    fixed_r = vector_r[:, None] * own_r + vector_i[:, None] * own_i
    fixed_i = vector_r[:, None] * own_i - vector_i[:, None] * own_r
    return jnp.stack([fixed_r, fixed_i])[:, None]


def unit_angles(top, n):
    angle = -2.0 * np.pi * (top % n) / n
    return np.cos(angle), np.sin(angle)


def halves(values):
    kind = jnp.dtype(BF16)
    high = values.astype(np.float32).astype(kind)
    low = (values - high.astype(np.float64)).astype(np.float32).astype(kind)
    return jnp.asarray(np.concatenate([high, high, low], axis=1))


def quarter_matrix(width):
    quarter = width // 4
    index = np.arange(quarter)
    real, imag = unit_angles(np.outer(index, index), quarter)
    return real / math.sqrt(width), imag / math.sqrt(width)


def column_tables(width):
    quarter = width // 4
    real, imag = quarter_matrix(width)
    twist = [unit_angles(np.arange(quarter) * k, width) for k in range(4)]
    turn = np.stack([t[0] for t in twist] + [t[1] for t in twist])
    return halves(np.concatenate([real, imag], axis=1)), jnp.asarray(turn, F32)


def row_tables(width, chunk, chunks, block):
    part = block // chunks
    lane = np.arange(2 * block)
    imaginary = lane % block >= part
    row = lane // block * block + chunk * part + lane % part
    real, imag = quarter_matrix(width)
    real, imag = real[:, row], imag[:, row]
    upper = np.where(imaginary, -imag, real)
    lower = np.where(imaginary, real, imag)
    twist = [unit_angles(row * k, width) for k in range(4)]
    sign = np.where(imaginary, 1.0, -1.0)
    turn = np.stack([t[0] for t in twist] + [t[1] * sign for t in twist])
    return halves(np.concatenate([upper, lower], axis=0)).T, jnp.asarray(turn, F32)


def split(value):
    high = value.astype(BF16)
    return high, (value - high.astype(F32)).astype(BF16)


def cost(micros):
    return pl.CostEstimate(flops=int(micros * 8e7), bytes_accessed=0, transcendentals=0)


def product(table, right):
    high, low = split(right)
    sides = jnp.concatenate([high, low, high], axis=1)
    return lax.dot_general(table, sides, (((1,), (1,)), ((), ())), preferred_element_type=F32)


def turn_kernel(me_ref, group_ref, phase_ref, refl_ref, own_ref, far_ref, send_ref, cos_ref, sin_ref, sum_ref):
    @pl.when(pl.program_id(0) == 0)
    def _():
        cos_ref[...] = jnp.cos(phase_ref[...])
        sin_ref[...] = jnp.sin(phase_ref[...])

    sum_ref[...] = jnp.zeros(sum_ref.shape, F32)
    count = refl_ref.shape[1]
    rows = refl_ref.shape[2]
    for f in range(count):
        slot = group_ref[f] ^ me_ref[0]
        cosine = cos_ref[f : f + 1, :]
        sine = sin_ref[f : f + 1, :]
        for t in range(0, rows, 8):
            real = refl_ref[0, f, t : t + 8, :]
            imag = refl_ref[1, f, t : t + 8, :]
            sum_r = sum_ref[slot, 0, t : t + 8, :]
            sum_i = sum_ref[slot, 1, t : t + 8, :]
            sum_ref[slot, 0, t : t + 8, :] = sum_r + (real * cosine - imag * sine)
            sum_ref[slot, 1, t : t + 8, :] = sum_i + (real * sine + imag * cosine)
    own_ref[...] = sum_ref[0]
    far_ref[...] = sum_ref[2]
    send_ref[0] = sum_ref[3]
    send_ref[1] = sum_ref[1]


def turn_sum(me, groups, phase, reflection, first, rows, rows_at):
    _, count, _, width = reflection.shape
    shape = jax.ShapeDtypeStruct((2, rows, width), F32)
    spec = pl.BlockSpec((2, rows_at, width), lambda i: (0, i, 0))
    offset = first // rows_at
    return pl.pallas_call(
        turn_kernel,
        grid=(rows // rows_at,),
        in_specs=[
            pl.BlockSpec(memory_space=pltpu.SMEM),
            pl.BlockSpec(memory_space=pltpu.SMEM),
            pl.BlockSpec((count, width), lambda i: (0, 0)),
            pl.BlockSpec((2, count, rows_at, width), lambda i: (0, 0, i + offset, 0)),
        ],
        out_specs=[spec, spec, pl.BlockSpec((2, 2, rows_at, width), lambda i: (0, 0, i, 0))],
        out_shape=[shape, shape, jax.ShapeDtypeStruct((2, 2, rows, width), F32)],
        scratch_shapes=[pltpu.VMEM((count, width), F32)] * 2 + [pltpu.VMEM((4, 2, rows_at, width), F32)],
        name="turn_sum",
        compiler_params=pltpu.CompilerParams(vmem_limit_bytes=56 * 2**20),
        cost_estimate=cost(4),
    )(me, groups, phase, reflection)


def columns_kernel(place_ref, table_ref, turn_ref, own_ref, far_ref, *refs):
    outs = refs[:-1]
    z_ref = refs[-1]
    rows, width = own_ref.shape[1:]
    quarter = width // 4
    block = width // (2 * len(outs))

    def plane(p):
        cuts = [slice(a * quarter, (a + 1) * quarter) for a in range(4)]
        return [own_ref[p, :, c] + far_ref[p, :, c] for c in cuts]

    a_r, b_r, c_r, d_r = plane(0)
    a_i, b_i, c_i, d_i = plane(1)
    s0_r, s0_i = a_r + c_r, a_i + c_i
    s1_r, s1_i = a_r - c_r, a_i - c_i
    s2_r, s2_i = b_r + d_r, b_i + d_i
    s3_r, s3_i = b_r - d_r, b_i - d_i
    mixed = (
        (s0_r + s2_r, s0_i + s2_i),
        (s1_r + s3_i, s1_i - s3_r),
        (s0_r - s2_r, s0_i - s2_i),
        (s1_r - s3_i, s1_i + s3_r),
    )
    for pair in range(2):
        stacked = []
        for k in (2 * pair, 2 * pair + 1):
            v_r, v_i = mixed[k]
            if k > 0:
                t_r = turn_ref[k : k + 1, :]
                t_i = turn_ref[4 + k : 5 + k, :]
                v_r, v_i = v_r * t_r - v_i * t_i, v_r * t_i + v_i * t_r
            stacked.append(jnp.concatenate([v_r, -v_i], axis=1))
            stacked.append(jnp.concatenate([v_i, v_r], axis=1))
        out = product(table_ref[...], jnp.concatenate(stacked, axis=0))
        for e in range(2):
            z_ref[pl.ds(2 * pair + e, quarter, stride=4), :] = out[:, 2 * rows * e : 2 * rows * (e + 1)]
    place = place_ref[0]
    for k in range(len(outs)):
        for p in range(2):
            start = pl.multiple_of((place ^ (2 * k + p)) * block, block)
            outs[k][p] = z_ref[pl.ds(start, block), :]


def columns_step(place, tables, own, far, spaces):
    _, rows, width = own.shape
    block = width // spaces
    return pl.pallas_call(
        columns_kernel,
        in_specs=[pl.BlockSpec(memory_space=pltpu.SMEM)] + [pl.BlockSpec(memory_space=pltpu.VMEM)] * 4,
        out_specs=[pl.BlockSpec(memory_space=pltpu.VMEM)] * (spaces // 2),
        out_shape=[jax.ShapeDtypeStruct((2, block, 2 * rows), F32)] * (spaces // 2),
        scratch_shapes=[pltpu.VMEM((width, 2 * rows), F32)],
        name="columns_step",
        compiler_params=pltpu.CompilerParams(vmem_limit_bytes=12 * 2**20),
        cost_estimate=cost(3),
    )(place, *tables, own, far)


def rows_kernel(origin_ref, table_ref, turn_ref, same_ref, cross_ref, *refs):
    out_ref, pieces_ref = refs[-2:]
    spaces, block, _ = pieces_ref.shape
    quarter = out_ref.shape[3]
    origin = origin_ref[0]
    for k in range(spaces // 2):
        pieces_ref[origin ^ (2 * k)] = same_ref[k]
        pieces_ref[origin ^ (2 * k + 1)] = cross_ref[k]
    half = block // 2
    lane = lax.broadcasted_iota(jnp.int32, (1, block), 1)
    sign = jnp.where(lane < half, 1.0, -1.0)

    def swap(x):
        return pltpu.roll(x, half, 1)

    def piece(s):
        return pieces_ref[s]

    mixed = [[], [], [], []]
    for e in range(2):
        a, b, c, d = [piece(2 * q + e) for q in range(4)]
        s0, s1, s2 = a + c, a - c, b + d
        s3 = swap(b - d) * sign
        for k, v in enumerate((s0 + s2, s1 + s3, s0 - s2, s1 - s3)):
            if k > 0:
                at = slice(e * block, (e + 1) * block)
                v = v * turn_ref[k : k + 1, at] + swap(v) * turn_ref[4 + k : 5 + k, at]
            mixed[k].append(v)
    for pair in range(2):
        stacked = [jnp.concatenate(mixed[k], axis=1) for k in (2 * pair, 2 * pair + 1)]
        high, low = split(jnp.concatenate(stacked, axis=0))
        out = jnp.dot(jnp.concatenate([high, low, high], axis=1), table_ref[...], preferred_element_type=F32)
        for e in range(2):
            for p in range(2):
                value = out[e * block : (e + 1) * block, p * quarter : (p + 1) * quarter]
                if len(refs) > 2:
                    value = value + refs[0][2 * pair + e, p]
                out_ref[2 * pair + e, p] = value


def rows_step(origin, tables, same, cross, *sofar):
    pairs, block, _ = same.shape
    width = 2 * pairs * block
    return pl.pallas_call(
        rows_kernel,
        in_specs=[pl.BlockSpec(memory_space=pltpu.SMEM)] + [pl.BlockSpec(memory_space=pltpu.VMEM)] * (4 + len(sofar)),
        out_specs=pl.BlockSpec(memory_space=pltpu.VMEM),
        out_shape=jax.ShapeDtypeStruct((4, 2, block, width // 4), F32),
        scratch_shapes=[pltpu.VMEM((2 * pairs, block, block), F32)],
        name="rows_step",
        compiler_params=pltpu.CompilerParams(vmem_limit_bytes=12 * 2**20),
        cost_estimate=cost(1),
    )(origin, *tables, same, cross, *sofar)


def focus_kernel(place_ref, origin_ref, widths_ref, table_ref, turn_ref, own_ref, near_ref, same_ref, cross_ref, *refs):
    sofar_ref, out_ref, other_ref, pieces_ref, vector_ref = refs
    rows_kernel(origin_ref, table_ref, turn_ref, same_ref, cross_ref, sofar_ref, other_ref, pieces_ref)
    _, _, block, quarter = own_ref.shape
    rows = 4 * quarter
    step = 128
    places = [(k, h) for k in range(4) for h in range(0, quarter, step)]
    near_left = place_ref[0] % 2

    def keep(top):
        position = top + lax.broadcasted_iota(jnp.int32, (8, 1), 0)
        left = (position >= block - widths_ref[0, 0]).astype(jnp.int32)
        right = (position < widths_ref[0, 1]).astype(jnp.int32)
        near = (left * near_left + right * (1 - near_left)).astype(F32)
        other = (right * near_left + left * (1 - near_left)).astype(F32)
        return near, other

    groups = []
    for top in range(0, block, 8):
        near, other = keep(top)
        groups += [(own_ref, top, None), (near_ref, top, near), (other_ref, top, other)]

    def plane(ref, top, p):
        return [ref[k, p, top : top + 8, h : h + step] for k, h in places]

    def normalize_rows(reals, imags):
        reals = [jnp.sum(x, axis=0, keepdims=True) for x in reals]
        imags = [jnp.sum(x, axis=0, keepdims=True) for x in imags]
        powers = [r * r + i * i for r, i in zip(reals, imags)]
        total = jnp.sum(sum(powers[1:], powers[0]), axis=1, keepdims=True)
        for t, power in enumerate(powers):
            scale = lax.rsqrt(power + total / rows + 1e-06)
            vector_ref[0, t : t + 1, :] = reals[t] * scale
            vector_ref[1, t : t + 1, :] = imags[t] * scale

    def vectors(p):
        return [jnp.broadcast_to(vector_ref[p, t : t + 1, :], (8, step)) for t in range(len(places))]

    zeros = [jnp.zeros((8, step), F32) for _ in places]
    real, imag = list(zeros), list(zeros)
    for ref, top, mask in groups:
        for total, p in ((real, 0), (imag, 1)):
            for t, x in enumerate(plane(ref, top, p)):
                total[t] = total[t] + (x if mask is None else x * mask)
    normalize_rows(real, imag)

    def iterate(_, carry):
        v_r, v_i = vectors(0), vectors(1)
        real, imag = list(zeros), list(zeros)
        for ref, top, mask in groups:
            r, i = plane(ref, top, 0), plane(ref, top, 1)
            b_r = sum(x * u + y * v for x, y, u, v in zip(r, i, v_r, v_i))
            b_i = sum(x * v - y * u for x, y, u, v in zip(r, i, v_r, v_i))
            b_r = jnp.sum(b_r, axis=1, keepdims=True)
            b_i = jnp.sum(b_i, axis=1, keepdims=True)
            if mask is not None:
                b_r, b_i = b_r * mask, b_i * mask
            b_r = jnp.broadcast_to(b_r, (8, step))
            b_i = jnp.broadcast_to(b_i, (8, step))
            for t in range(len(places)):
                real[t] = real[t] + (r[t] * b_r - i[t] * b_i)
                imag[t] = imag[t] + (r[t] * b_i + i[t] * b_r)
        normalize_rows(real, imag)
        return carry

    lax.fori_loop(0, ITERS, iterate, 0)
    for t, (k, h) in enumerate(places):
        r = own_ref[k, 0, :, h : h + step]
        i = own_ref[k, 1, :, h : h + step]
        v_r = vector_ref[0, t : t + 1, :]
        v_i = vector_ref[1, t : t + 1, :]
        at = pl.ds(4 * h + k, step, stride=4)
        out_ref[0, 0, at, :] = (v_r * r + v_i * i).T
        out_ref[1, 0, at, :] = (v_r * i - v_i * r).T


def focus_step(place, origin, widths, tables, own, near, same, cross, sofar):
    _, _, block, quarter = own.shape
    rows = 4 * quarter
    smem = pl.BlockSpec(memory_space=pltpu.SMEM)
    vmem = pl.BlockSpec(memory_space=pltpu.VMEM)
    return pl.pallas_call(
        focus_kernel,
        in_specs=[smem] * 3 + [vmem] * 7,
        out_specs=vmem,
        out_shape=jax.ShapeDtypeStruct((2, 1, rows, block), F32),
        scratch_shapes=[
            pltpu.VMEM(own.shape, F32),
            pltpu.VMEM((rows // block, block, block), F32),
            pltpu.VMEM((2, rows // 128, 128), F32),
        ],
        name="focus_step",
        compiler_params=pltpu.CompilerParams(vmem_limit_bytes=16 * 2**20),
        cost_estimate=cost(6),
    )(place, origin, widths, *tables, own, near, same, cross, sofar)


CHUNKS = 2


def local(reflection, phase, group_index, widths):
    return focus_all(reflection, phase, group_index, widths)


def focus_all(reflection, phase, group_index, widths):
    rows_here, width = reflection.shape[2:]
    count = lax.axis_size("freq")
    spaces = lax.axis_size("space")
    block = width // spaces
    me = lax.axis_index("freq").astype(jnp.int32)[None]
    place = lax.axis_index("space").astype(jnp.int32)[None]
    near = [(i, i ^ 1) for i in range(count)]
    far = [(i, i ^ 2) for i in range(count)]
    along = [(i, (i + 2 if i % 2 == 0 else i - 2) % spaces) for i in range(spaces)]
    beyond_from = jnp.where(place % 2 == 0, place + (spaces - 2), place + 2) % spaces
    columns = column_tables(width)
    chunk = rows_here // CHUNKS
    cores, fars, mine = [], [], []
    sums = []
    for h in range(CHUNKS):
        sums.append(turn_sum(me, group_index, phase, reflection, h * chunk, chunk, 32))
        cores.append(lax.ppermute(sums[h][2], "freq", near))
        partial = sums[h][1] + cores[h][0]
        mine.append(sums[h][0] + cores[h][1])
        fars.append(lax.ppermute(partial, "freq", far))
    own_block = near_block = other_block = ()
    for h in range(CHUNKS):
        rows = row_tables(width, h, CHUNKS, block)
        pieces = list(columns_step(place, columns, mine[h], fars[h], spaces))
        for k in range(1, spaces // 2):
            pieces[k] = lax.ppermute(pieces[k], "space", [(i, i ^ (2 * k)) for i in range(spaces)])
        own_same, near_same = [jnp.stack([piece[p] for piece in pieces]) for p in range(2)]
        across = [(i, i ^ 1) for i in range(spaces)]
        near_cross = lax.ppermute(own_same, "space", across)
        own_cross = lax.ppermute(near_same, "space", across)
        beyond = lax.ppermute(jnp.stack([near_same, near_cross]), "space", along)
        own_block = (rows_step(place, rows, own_same, own_cross, *own_block),)
        near_block = (rows_step(place, rows, near_same, near_cross, *near_block),)
        if h + 1 < CHUNKS:
            other_block = (rows_step(beyond_from, rows, beyond[0], beyond[1], *other_block),)
    return focus_step(
        place, beyond_from, widths, rows, own_block[0], near_block[0], beyond[0], beyond[1], other_block[0]
    )


def solution(mesh):
    in_specs = (P(None, "freq", "space", None), P("freq", None), P("freq"), P("space", None))
    out_specs = P(None, "freq", None, "space")

    def step(reflection, phase, group_index, widths):
        block = reflection.shape[3] // mesh.shape["space"]
        rows = reflection.shape[2] // mesh.shape["space"]
        whole = block % 128 == 0 and rows == 128 and mesh.shape["freq"] == 4 and mesh.shape["space"] == 8
        body = local if whole else plain_local
        return jax.shard_map(
            body, mesh=mesh, in_specs=in_specs, out_specs=out_specs, check_vma=False
        )(reflection, phase, group_index, widths)

    return step
```
